256 devices in a mesh: dom: 256 (over x, y, z, core).
Axes of the slice: x: 4, y: 4, z: 8, core: 2. Of those that a mesh axis runs over, the one named last changes fastest.
Arguments:
- features: bfloat16 [262144, 512], P('dom'), may hold values from -6 to 6
- embeddings: bfloat16 [262144, 128], P('dom'), may hold values from -6 to 6
- tile_values: bfloat16 [2048, 4, 128, 128], P('dom'), may hold values from -4 to 4
- tile_columns: int32 [2048, 4], P('dom'), may hold values from 0 to 11
- send_blocks: int32 [256, 2, 2], P('dom'), may hold values from 0 to 7
- send_count: int32 [256, 2], P('dom'), may hold values from 1 to 2, as said below
- hub_rows: int32 [512], P('dom'), may hold values from 0 to 1023, as said below
- hub_weight: bfloat16 [262144, 512], P('dom'), may hold values from -4 to 4
- degree: int32 [262144], P('dom'), may hold values from 16 to 64
Outputs:
- hop_features: bfloat16 [3, 262144, 512], P(None, 'dom')
- hop_embeddings: bfloat16 [3, 262144, 128], P(None, 'dom')
The draws below stay inside these ranges and needn't reach their ends.
Inputs may be any that keep to these rules, and one draw needn't show every extreme that they name: `send_count`: some partition sends 2 blocks to its right and some to its left. `hub_rows`: the 2 hub rows of each partition are distinct local row numbers.
All inputs are finite; a program needn't handle non-finite values.
Results may differ from the reference program's by a relative error of at most 0.012.
Values may be sent and summed in bfloat16 or wider, within the bound.
A program may use at most 64 MiB of HBM per device.

```python
import jax
import jax.numpy as jnp
from jax import lax

F = 512
E = 128
TILE = 128
ROWS_DEV = 1024
K = 4
SEND_MOST = 2
HUB_DEV = 2
HOPS = 3
ROWS = 262144
BLOCKS = 2048
HUBS = 512
N_DOM = 256


def draw_send_count(key, part):
    counts = jax.random.randint(key, (N_DOM, 2), 1, SEND_MOST + 1)
    counts = counts.at[0, 1].set(SEND_MOST)
    counts = counts.at[N_DOM - 1, 0].set(SEND_MOST)
    return counts.astype(jnp.int32)


def draw_hub_rows(key, part):

    def one_device(device_index):
        return jax.random.permutation(jax.random.fold_in(key, device_index), ROWS_DEV)[:HUB_DEV]
    chosen = jax.vmap(one_device)(jnp.arange(N_DOM, dtype=jnp.int32))
    return chosen.reshape(-1).astype(jnp.int32)


def plant(array, stream_key, least, high):
    spot = [jax.random.randint(jax.random.fold_in(stream_key, axis), (), 0, length) for axis, length in enumerate(array.shape)]
    longest = array.shape.index(max(array.shape))
    next_to = spot[:longest] + [(spot[longest] + 1) % array.shape[longest]] + spot[longest + 1:]
    return array.at[tuple(spot)].set(least).at[tuple(next_to)].set(high)


def block_scale(own_key, shape, cuts, low, top_value):
    def one(dim, blocks):
        steps = jax.random.uniform(jax.random.fold_in(jax.random.fold_in(own_key, 6), dim), (blocks,), jnp.float32, low / len(cuts), top_value / len(cuts))
        return jnp.repeat(jnp.exp(steps), shape[dim] // blocks).reshape((-1,) + (1,) * (len(shape) - dim - 1))

    level = one(*cuts[0])
    for cut in cuts[1:]:
        level = level * one(*cut)
    return level


def scatter_about(rng, dims, spread, reach, pieces=(), kind=jnp.bfloat16):
    values = spread * jax.random.normal(rng, dims, jnp.float32)
    if pieces:
        values = values * block_scale(rng, dims, pieces, -0.22, 0.18)
    return jnp.clip(values, -reach, reach).astype(kind)


def setup_inputs(seed: int = 0) -> dict:
    key_of = jax.random.split(jax.random.key(seed), 10)
    features = scatter_about(key_of[0], (ROWS, F), 1.0, 6.0, ((0, 256),))
    embeddings = scatter_about(key_of[1], (ROWS, E), 1.0, 6.0, ((0, 256),))
    tile_values = scatter_about(key_of[2], (BLOCKS, K, TILE, TILE), 1.0, 4.0, ((0, 256),))
    tile_columns = plant(jax.random.randint(key_of[3], (BLOCKS, K), 0, ROWS_DEV // TILE + 2 * SEND_MOST), jax.random.fold_in(key_of[3], 1), 0, (ROWS_DEV // TILE + 2 * SEND_MOST) - 1).astype(jnp.int32)
    send_blocks = plant(jax.random.randint(key_of[4], (N_DOM, 2, SEND_MOST), 0, ROWS_DEV // TILE), jax.random.fold_in(key_of[4], 1), 0, (ROWS_DEV // TILE) - 1).astype(jnp.int32)
    send_count = draw_send_count(jax.random.fold_in(key_of[9], 71), 0)
    hub_rows = draw_hub_rows(jax.random.fold_in(key_of[9], 71), 0)
    hub_weight = scatter_about(key_of[7], (ROWS, HUBS), 1.0, 4.0, ((0, 256),))
    degree = plant(jax.random.randint(key_of[8], (ROWS,), 16, 65), jax.random.fold_in(key_of[8], 1), 16, 64).astype(jnp.int32)
    return {"features": features, "embeddings": embeddings, "tile_values": tile_values, "tile_columns": tile_columns, "send_blocks": send_blocks, "send_count": send_count, "hub_rows": hub_rows, "hub_weight": hub_weight, "degree": degree}


def reference(features, embeddings, tile_values, tile_columns, send_blocks, send_count, hub_rows, hub_weight, degree):
    feature_width = F + E
    block_count = ROWS_DEV // TILE
    device_count = N_DOM
    inverse_root = lax.rsqrt(degree.astype(jnp.float32)).reshape(device_count, ROWS_DEV, 1)
    current = jnp.concatenate([features, embeddings], axis=1).reshape(device_count, ROWS_DEV, feature_width)
    tiles_split = tile_values.reshape(device_count, block_count, K, TILE, TILE)
    columns_split = tile_columns.reshape(device_count, block_count, K).astype(jnp.int32)
    hubs_split = hub_rows.reshape(device_count, HUB_DEV).astype(jnp.int32)
    weight_split = hub_weight.reshape(device_count, ROWS_DEV, HUBS)
    live_slots = jnp.arange(SEND_MOST, dtype=jnp.int32)[None, None, :] < send_count[:, :, None]
    empty_rim = jnp.zeros((1, SEND_MOST, TILE, feature_width), jnp.bfloat16)
    results = []
    for hop_index in range(HOPS):
        scaled = (current.astype(jnp.float32) * inverse_root).astype(jnp.bfloat16)
        blocked = scaled.reshape(device_count, block_count, TILE, feature_width)
        outgoing = jax.vmap(lambda source, listed: source[listed])(blocked, send_blocks.astype(jnp.int32))
        outgoing = jnp.where(live_slots[:, :, :, None, None], outgoing, jnp.zeros_like(outgoing))
        from_left = jnp.concatenate([empty_rim, outgoing[:-1, 1]], axis=0)
        from_right = jnp.concatenate([outgoing[1:, 0], empty_rim], axis=0)
        extended = jnp.concatenate([blocked, from_left, from_right], axis=1)
        gathered_hubs = jax.vmap(lambda source, listed: source[listed])(scaled, hubs_split).reshape(HUBS, feature_width)

        def one_device(operands):
            buffer, tiles_here, columns_here, weight_here = operands
            picked = buffer[columns_here]
            local_part = jnp.einsum('bkij,bkjw->biw', tiles_here.astype(jnp.float32), picked.astype(jnp.float32))
            local_part = local_part.reshape(ROWS_DEV, feature_width)
            return local_part + jnp.dot(weight_here, gathered_hubs, preferred_element_type=jnp.float32)
        summed = lax.map(one_device, (extended, tiles_split, columns_split, weight_split))
        current = (summed * inverse_root).astype(jnp.bfloat16)
        results.append(current.reshape(ROWS, feature_width))
    stacked = jnp.stack(results)
    return (stacked[:, :, :F], stacked[:, :, F:])
```

```python
import jax
import jax.numpy as jnp
from jax import lax
from jax.experimental import pallas as pl
from jax.experimental.pallas import tpu as pltpu
from jax.sharding import PartitionSpec as P

HOPS = 3
NX, NY, NZ = 4, 4, 8
NG = NX * NY
N_DOM = NG * NZ * 2
HALF_Z = NZ // 2
TILE = 128
ROWS = 1024
BLOCKS = 8
K = 4
F, E = 512, 128
WIDTH = F + E
HUBS = 512
CHUNKS = ((0, 256), (256, 256), (512, 128))
BF16, F32 = jnp.bfloat16, jnp.float32


def kernel(
    feat, emb, tv_hbm, w_hbm, deg, cols, sblk, scnt, hubs,
    outf, oute,
    xf, xe, tv, wv, inv, zs, ext0, ext1, ext2, halo, acc, xo, hsend, land, tsend, gbuf,
    in_sem, hs_sem, hr_sem, s1, r1, s2, r2, s3, r3, out_sem,
):
    exts = (ext0, ext1, ext2)
    me = lax.axis_index("dom")
    core = lax.rem(me, 2)
    z = lax.rem(lax.div(me, 2), NZ)
    g = lax.div(me, 2 * NZ)
    gx = lax.div(g, NY)
    gy = lax.rem(g, NY)
    partner = me + 1 - 2 * core
    cls = lax.div(z, HALF_Z)
    own_slot = lax.rem(z, HALF_Z) * 2 + core

    def dev(g_, z_, c_):
        return (g_ * NZ + z_) * 2 + c_

    def plane(d):
        x_ = lax.rem(gx + lax.div(d, NY), NX)
        y_ = lax.rem(gy + lax.rem(d, NY), NY)
        return x_ * NY + y_

    loads = [
        pltpu.make_async_copy(feat, xf, in_sem.at[0]),
        pltpu.make_async_copy(emb, xe, in_sem.at[1]),
        pltpu.make_async_copy(tv_hbm, tv, in_sem.at[2]),
        pltpu.make_async_copy(w_hbm, wv, in_sem.at[3]),
    ]
    for load in loads:
        load.start()

    barrier = pltpu.get_barrier_semaphore()

    @pl.loop(1, 2 * NZ)
    def _(d):
        pl.semaphore_signal(barrier, inc=1, device_id={"dom": g * 2 * NZ + lax.rem(z * 2 + core + d, 2 * NZ)})

    @pl.loop(1, NG)
    def _(d):
        pl.semaphore_signal(barrier, inc=1, device_id={"dom": dev(plane(d), z, core)})

    @pl.when(me > 0)
    def _():
        pl.semaphore_signal(barrier, inc=1, device_id={"dom": me - 1})

    @pl.when(me < N_DOM - 1)
    def _():
        pl.semaphore_signal(barrier, inc=1, device_id={"dom": me + 1})

    root = lax.rsqrt(deg[...].astype(F32))
    for b in range(BLOCKS):
        inv[b] = jnp.broadcast_to(root[b : b + 1, :], (TILE, TILE)).T

    @pl.when(me == 0)
    def _():
        for h in range(HOPS):
            exts[h][8:10] = jnp.zeros((2, TILE, WIDTH), BF16)

    @pl.when(me == N_DOM - 1)
    def _():
        for h in range(HOPS):
            exts[h][10:12] = jnp.zeros((2, TILE, WIDTH), BF16)

    loads[0].wait()
    loads[1].wait()

    @pl.loop(0, BLOCKS)
    def _(b):
        rows = pl.ds(pl.multiple_of(b * TILE, TILE), TILE)
        scale = inv[b]
        for j in range(F // TILE):
            lanes = slice(j * TILE, (j + 1) * TILE)
            scaled = (xf[rows, lanes].astype(F32) * scale).astype(BF16)
            zs[b, :, lanes] = scaled
            ext0[b, :, lanes] = scaled
        scaled = (xe[rows, :].astype(F32) * scale).astype(BF16)
        zs[b, :, F:] = scaled
        ext0[b, :, F:] = scaled

    def barrier_wait():
        extra = jnp.where(me > 0, 1, 0) + jnp.where(me < N_DOM - 1, 1, 0)
        pl.semaphore_wait(barrier, 2 * NZ - 1 + NG - 1 + extra)

    def first_copy(h, d):
        q = dev(g, lax.rem(z + d, NZ), cls)
        return q, pltpu.make_async_remote_copy(
            src_ref=hsend.at[h], dst_ref=land.at[h, own_slot], send_sem=s1.at[h, d], recv_sem=r1.at[h, own_slot],
            device_id={"dom": q}, device_id_type=pl.DeviceIdType.MESH)

    def second_copy(h, d):
        return pltpu.make_async_remote_copy(
            src_ref=tsend.at[h], dst_ref=gbuf.at[h, g, core], send_sem=s2.at[h, d], recv_sem=r2.at[h, g],
            device_id={"dom": dev(plane(d), z, core)}, device_id_type=pl.DeviceIdType.MESH)

    def arrival(h, d):
        src = plane(d)
        return src, pltpu.make_async_remote_copy(
            src_ref=tsend.at[h], dst_ref=gbuf.at[h, src, core], send_sem=s2.at[h, d], recv_sem=r2.at[h, src],
            device_id={"dom": dev(src, z, core)}, device_id_type=pl.DeviceIdType.MESH)

    def third_copy(h, src, lane):
        return pltpu.make_async_remote_copy(
            src_ref=gbuf.at[h, src, lane], dst_ref=gbuf.at[h, src, lane], send_sem=s3.at[h, src], recv_sem=r3.at[h, src],
            device_id={"dom": partner}, device_id_type=pl.DeviceIdType.MESH)

    def to_left(h):
        return pltpu.make_async_remote_copy(
            src_ref=halo.at[h, 0], dst_ref=exts[h].at[10:12], send_sem=hs_sem.at[h, 0], recv_sem=hr_sem.at[h, 0],
            device_id={"dom": me - 1}, device_id_type=pl.DeviceIdType.MESH)

    def to_right(h):
        return pltpu.make_async_remote_copy(
            src_ref=halo.at[h, 1], dst_ref=exts[h].at[8:10], send_sem=hs_sem.at[h, 1], recv_sem=hr_sem.at[h, 1],
            device_id={"dom": me + 1}, device_id_type=pl.DeviceIdType.MESH)

    for h in range(HOPS):
        picked = []
        for i in range(2):
            r = hubs[i]
            b = lax.shift_right_logical(r, 7)
            rows = zs[b].astype(F32)
            hit = lax.broadcasted_iota(jnp.int32, (TILE, WIDTH), 0) == jnp.bitwise_and(r, TILE - 1)
            picked.append(jnp.sum(jnp.where(hit, rows, 0.0), axis=0, keepdims=True))
        pair = jnp.concatenate(picked, axis=0).astype(BF16)
        hsend[h] = pair
        for j in range(2):
            for s in range(2):
                block = zs[sblk[0, j, s]]
                live = lax.broadcasted_iota(jnp.int32, (TILE, WIDTH), 0) * 0 + s < scnt[0, j]
                halo[h, j, s] = jnp.where(live, block.astype(F32), 0.0).astype(BF16)
        if h == 0:
            barrier_wait()

        @pl.loop(0, NZ)
        def _(d):
            q, copy = first_copy(h, d)

            @pl.when(q != me)
            def _():
                copy.start()

        @pl.when(cls == core)
        def _():
            land[h, own_slot] = pair

        @pl.when(me > 0)
        def _():
            to_left(h).start()

        @pl.when(me < N_DOM - 1)
        def _():
            to_right(h).start()

        for s in range(NZ):
            source = dev(g, core * HALF_Z + s // 2, s % 2)

            @pl.when(source != me)
            def _():
                pltpu.make_async_remote_copy(
                    src_ref=hsend.at[h], dst_ref=land.at[h, s], send_sem=s1.at[h, s], recv_sem=r1.at[h, s],
                    device_id={"dom": source}, device_id_type=pl.DeviceIdType.MESH).wait_recv()

        whole = jnp.concatenate([land[h, s].astype(F32) for s in range(NZ)], axis=0).astype(BF16)
        tsend[h] = whole
        gbuf[h, g, core] = whole

        @pl.loop(1, NG)
        def _(d):
            second_copy(h, d).start()

        third_copy(h, g, core).start()
        if h == 0:
            loads[2].wait()
            loads[3].wait()

        @pl.when(me > 0)
        def _():
            to_right(h).wait_recv()

        @pl.when(me < N_DOM - 1)
        def _():
            to_left(h).wait_recv()

        @pl.loop(0, BLOCKS)
        def _(b):
            left = jnp.concatenate([tv[b, k] for k in range(K)], axis=1)
            right = jnp.concatenate([exts[h][cols[k, b]] for k in range(K)], axis=0)
            acc[b] = jnp.dot(left, right, preferred_element_type=F32)
            for e in range(2):
                d = 2 * b + e

                @pl.when(d > 0)
                def _():
                    src, landed = arrival(h, d)
                    landed.wait_recv()
                    third_copy(h, src, core).start()

        @pl.loop(0, NG)
        def _(src):
            third_copy(h, src, 1 - core).wait_recv()

        for first, count in CHUNKS:
            lanes = slice(first, first + count)
            hub_part = gbuf[h, :, :, :, lanes].reshape(HUBS, count)

            @pl.loop(0, 2)
            def _(half):
                rows = pl.ds(pl.multiple_of(half * 512, 512), 512)
                prod = jnp.dot(wv[rows, :], hub_part, preferred_element_type=F32)
                for q in range(4):
                    b = half * 4 + q
                    scale = inv[b]
                    for j in range(count // TILE):
                        at = slice(first + j * TILE, first + (j + 1) * TILE)
                        y = acc[b, :, at] + prod[q * TILE : (q + 1) * TILE, j * TILE : (j + 1) * TILE]
                        x = (y * scale).astype(BF16)
                        xo[h, pl.ds(pl.multiple_of(b * TILE, TILE), TILE), at] = x
                        if h < HOPS - 1:
                            scaled = (x.astype(F32) * scale).astype(BF16)
                            zs[b, :, at] = scaled
                            exts[h + 1][b, :, at] = scaled

        pltpu.make_async_copy(xo.at[h, :, :F], outf.at[h], out_sem.at[h, 0]).start()
        pltpu.make_async_copy(xo.at[h, :, F:], oute.at[h], out_sem.at[h, 1]).start()

    for h in range(HOPS):
        @pl.loop(0, NZ)
        def _(d):
            q, copy = first_copy(h, d)

            @pl.when(q != me)
            def _():
                copy.wait_send()

        @pl.loop(1, NG)
        def _(d):
            second_copy(h, d).wait_send()

        @pl.loop(0, NG)
        def _(src):
            third_copy(h, src, core).wait_send()

        @pl.when(me > 0)
        def _():
            to_left(h).wait_send()

        @pl.when(me < N_DOM - 1)
        def _():
            to_right(h).wait_send()

        pltpu.make_async_copy(xo.at[h, :, :F], outf.at[h], out_sem.at[h, 0]).wait()
        pltpu.make_async_copy(xo.at[h, :, F:], oute.at[h], out_sem.at[h, 1]).wait()


def body(features, embeddings, tile_values, tile_columns, send_blocks, send_count, hub_rows, hub_weight, degree):
    hbm = pl.BlockSpec(memory_space=pl.ANY)
    vmem = pl.BlockSpec(memory_space=pltpu.VMEM)
    smem = pl.BlockSpec(memory_space=pltpu.SMEM)
    dma = pltpu.SemaphoreType.DMA
    return pl.pallas_call(
        kernel,
        out_shape=(
            jax.ShapeDtypeStruct((HOPS, ROWS, F), BF16),
            jax.ShapeDtypeStruct((HOPS, ROWS, E), BF16),
        ),
        in_specs=[hbm, hbm, hbm, hbm, vmem, smem, smem, smem, smem],
        out_specs=(hbm, hbm),
        scratch_shapes=[
            pltpu.VMEM((ROWS, F), BF16),
            pltpu.VMEM((ROWS, E), BF16),
            pltpu.VMEM((BLOCKS, K, TILE, TILE), BF16),
            pltpu.VMEM((ROWS, HUBS), BF16),
            pltpu.VMEM((BLOCKS, TILE, TILE), F32),
            pltpu.VMEM((BLOCKS, TILE, WIDTH), BF16),
            pltpu.VMEM((12, TILE, WIDTH), BF16),
            pltpu.VMEM((12, TILE, WIDTH), BF16),
            pltpu.VMEM((12, TILE, WIDTH), BF16),
            pltpu.VMEM((HOPS, 2, 2, TILE, WIDTH), BF16),
            pltpu.VMEM((BLOCKS, TILE, WIDTH), F32),
            pltpu.VMEM((HOPS, ROWS, WIDTH), BF16),
            pltpu.VMEM((HOPS, 2, WIDTH), BF16),
            pltpu.VMEM((HOPS, NZ, 2, WIDTH), BF16),
            pltpu.VMEM((HOPS, 16, WIDTH), BF16),
            pltpu.VMEM((HOPS, NG, 2, 16, WIDTH), BF16),
            dma((4,)),
            dma((HOPS, 2)),
            dma((HOPS, 2)),
            dma((HOPS, NZ)),
            dma((HOPS, NZ)),
            dma((HOPS, NG)),
            dma((HOPS, NG)),
            dma((HOPS, NG)),
            dma((HOPS, NG)),
            dma((HOPS, 2)),
        ],
        compiler_params=pltpu.CompilerParams(
            collective_id=0, has_side_effects=True, vmem_limit_bytes=60 * 1024 * 1024
        ),
        name="hops",
    )(features, embeddings, tile_values, hub_weight, degree.reshape(8, 128), tile_columns.T, send_blocks, send_count, hub_rows)


def solution(mesh):
    dom = P("dom", None)
    placed = (dom, dom, P("dom", None, None, None), dom, P("dom", None, None), dom, P("dom"), dom, P("dom"))
    return jax.shard_map(
        body,
        mesh=mesh,
        in_specs=placed,
        out_specs=(P(None, "dom", None), P(None, "dom", None)),
        check_vma=False,
    )
```

```python
import jax
import jax.numpy as jnp
from jax import lax
from jax.experimental import pallas as pl
from jax.experimental.pallas import tpu as pltpu
from jax.sharding import PartitionSpec as P

HOPS = 3
NX, NY, NZ = 4, 4, 8
NG = NX * NY
N_DOM = NG * NZ * 2
HALF_Z = NZ // 2
TILE = 128
ROWS = 1024
BLOCKS = 8
K = 4
F, E = 512, 128
WIDTH = F + E
HUBS = 512
CHUNKS = ((0, 256), (256, 256), (512, 128))
LANES = tuple(slice(first, first + count) for first, count in CHUNKS)
FAR_FIRST = (10, 6, 9, 11, 14, 2, 8, 5, 7, 13, 15, 1, 3, 4, 12)
RING_FAR_FIRST = (4, 3, 5, 2, 6, 1, 7, 0)
BF16, F32 = jnp.bfloat16, jnp.float32


def kernel(
    feat, emb, tv_hbm, w_hbm, deg_hbm, cols_hbm, sblk_hbm, scnt_hbm, hubs_hbm,
    xo, wv, inv, acc, gbuf2,
    deg, cols, sblk, scnt, hubs, xf, xe, tv, e00, e01, e02, e10, e11, e12, e20, e21, e22, halo, hsend, land, tsend, gbuf0, gbuf1,
    in_sem, hs_sem, hr_sem, s1, r1, s2, r2, s3, r3,
):
    exts = ((e00, e01, e02), (e10, e11, e12), (e20, e21, e22))
    gbufs = (gbuf0, gbuf1, gbuf2)
    me = lax.axis_index("dom")
    core = lax.rem(me, 2)
    z = lax.rem(lax.div(me, 2), NZ)
    g = lax.div(me, 2 * NZ)
    gx = lax.div(g, NY)
    gy = lax.rem(g, NY)
    partner = me + 1 - 2 * core
    cls = lax.div(z, HALF_Z)
    own_slot = lax.rem(z, HALF_Z) * 2 + core

    def dev(g_, z_, c_):
        return (g_ * NZ + z_) * 2 + c_

    def plane(d):
        x_ = lax.rem(gx + lax.div(d, NY), NX)
        y_ = lax.rem(gy + lax.rem(d, NY), NY)
        return x_ * NY + y_

    def remote(src, dst, send, recv, q):
        return pltpu.make_async_remote_copy(
            src_ref=src, dst_ref=dst, send_sem=send, recv_sem=recv,
            device_id={"dom": q}, device_id_type=pl.DeviceIdType.MESH)

    def first_copy(h, d):
        q = dev(g, lax.rem(z + d, NZ), cls)
        return q, remote(hsend.at[h], land.at[h, own_slot], s1.at[h, d], r1.at[h, own_slot], q)

    def second_copy(h, d):
        return remote(tsend.at[h], gbufs[h].at[g, core], s2.at[h, d], r2.at[h, g], dev(plane(d), z, core))

    def arrival(h, d):
        src = plane(d)
        return src, remote(tsend.at[h], gbufs[h].at[src, core], s2.at[h, d], r2.at[h, src], dev(src, z, core))

    def third_copy(h, src, lane):
        return remote(gbufs[h].at[src, lane], gbufs[h].at[src, lane], s3.at[h, src], r3.at[h, src], partner)

    def to_left(h, n):
        return remote(halo.at[h, 0, :, :, LANES[n]], exts[h][n].at[10:12], hs_sem.at[h, 0, n], hr_sem.at[h, 0, n], me - 1)

    def to_right(h, n):
        return remote(halo.at[h, 1, :, :, LANES[n]], exts[h][n].at[8:10], hs_sem.at[h, 1, n], hr_sem.at[h, 1, n], me + 1)

    small = [
        pltpu.make_async_copy(src, dst, in_sem.at[4 + i])
        for i, (src, dst) in enumerate(
            ((deg_hbm, deg), (cols_hbm, cols), (sblk_hbm, sblk), (scnt_hbm, scnt), (hubs_hbm, hubs)))
    ]
    loads = [
        pltpu.make_async_copy(feat, xf, in_sem.at[0]),
        pltpu.make_async_copy(emb, xe, in_sem.at[1]),
        pltpu.make_async_copy(w_hbm, wv, in_sem.at[2]),
        pltpu.make_async_copy(tv_hbm, tv, in_sem.at[3]),
    ]
    for load in small + loads:
        load.start()

    barrier = pltpu.get_barrier_semaphore()

    @pl.loop(1, 2 * NZ)
    def _(d):
        pl.semaphore_signal(barrier, inc=1, device_id={"dom": g * 2 * NZ + lax.rem(z * 2 + core + d, 2 * NZ)})

    @pl.loop(1, NG)
    def _(d):
        pl.semaphore_signal(barrier, inc=1, device_id={"dom": dev(plane(d), z, core)})

    @pl.when(me > 0)
    def _():
        pl.semaphore_signal(barrier, inc=1, device_id={"dom": me - 1})

    @pl.when(me < N_DOM - 1)
    def _():
        pl.semaphore_signal(barrier, inc=1, device_id={"dom": me + 1})

    def barrier_wait():
        extra = jnp.where(me > 0, 1, 0) + jnp.where(me < N_DOM - 1, 1, 0)
        pl.semaphore_wait(barrier, 2 * NZ - 1 + NG - 1 + extra)

    for load in small:
        load.wait()
    root = lax.rsqrt(deg[...].astype(F32))
    for b in range(BLOCKS):
        inv[b] = jnp.broadcast_to(root[b : b + 1, :], (TILE, TILE)).T

    @pl.when(me == 0)
    def _():
        for h in range(HOPS):
            for n, (_, count) in enumerate(CHUNKS):
                exts[h][n][8:10] = jnp.zeros((2, TILE, count), BF16)

    @pl.when(me == N_DOM - 1)
    def _():
        for h in range(HOPS):
            for n, (_, count) in enumerate(CHUNKS):
                exts[h][n][10:12] = jnp.zeros((2, TILE, count), BF16)

    hub_block = [lax.shift_right_logical(hubs[i], 7) for i in range(2)]
    hub_in = [jnp.bitwise_and(hubs[i], TILE - 1) for i in range(2)]

    def pick(ref):
        rows = []
        for i in range(2):
            block = ref[hub_block[i]].astype(F32)
            hit = lax.broadcasted_iota(jnp.int32, block.shape, 0) == hub_in[i]
            rows.append(jnp.sum(jnp.where(hit, block, 0.0), axis=0, keepdims=True))
        return jnp.concatenate(rows, axis=0)

    def times(block, scale):
        width = block.shape[-1]
        return jnp.concatenate([block[:, j : j + TILE] * scale for j in range(0, width, TILE)], axis=1)

    def send_first(h, pair):
        hsend[h] = pair
        if h == 0:
            barrier_wait()

        for d in RING_FAR_FIRST:
            q, copy = first_copy(h, d)

            @pl.when(q != me)
            def _():
                copy.start()

        @pl.when(cls == core)
        def _():
            land[h, own_slot] = pair

    def listed(j, s, width):
        live = lax.broadcasted_iota(jnp.int32, (TILE, width), 0) * 0 + s < scnt[0, j]
        return sblk[0, j, s], live

    def send_halo(h, n):
        @pl.when(me > 0)
        def _():
            to_left(h, n).start()

        @pl.when(me < N_DOM - 1)
        def _():
            to_right(h, n).start()

    hub_scale = pick(inv)
    loads[0].wait()
    loads[1].wait()
    first = jnp.concatenate([pick(xf), pick(xe)], axis=1)
    send_first(0, times(first, hub_scale).astype(BF16))
    for n, (at, count) in enumerate(CHUNKS):
        for j in range(2):
            for s in range(2):
                b, live = listed(j, s, count)
                block = xf[b, :, LANES[n]] if at < F else xe[b]
                halo[0, j, s, :, LANES[n]] = jnp.where(live, times(block.astype(F32), inv[b]), 0.0).astype(BF16)
        send_halo(0, n)

    @pl.loop(0, BLOCKS)
    def _(b):
        scale = inv[b]
        for n, (at, count) in enumerate(CHUNKS):
            block = xf[b, :, LANES[n]] if at < F else xe[b]
            exts[0][n][b] = times(block.astype(F32), scale).astype(BF16)

    loads[2].wait()
    loads[3].wait()
    hub_w = jnp.concatenate([pick(wv), jnp.zeros((14, HUBS), F32)], axis=0).astype(BF16)

    for h in range(HOPS):
        for s in range(NZ):
            source = dev(g, core * HALF_Z + s // 2, s % 2)

            @pl.when(source != me)
            def _():
                remote(hsend.at[h], land.at[h, s], s1.at[h, s], r1.at[h, s], source).wait_recv()

        whole = jnp.concatenate([land[h, s].astype(F32) for s in range(NZ)], axis=0).astype(BF16)
        tsend[h] = whole
        gbufs[h][g, core] = whole

        for d in FAR_FIRST:
            second_copy(h, d).start()
        third_copy(h, g, core).start()

        for n, (at, count) in enumerate(CHUNKS):
            @pl.when(me > 0)
            def _():
                to_right(h, n).wait_recv()

            @pl.when(me < N_DOM - 1)
            def _():
                to_left(h, n).wait_recv()

            @pl.loop(0, BLOCKS)
            def _(b):
                left = jnp.concatenate([tv[b, k] for k in range(K)], axis=1)
                right = jnp.concatenate([exts[h][n][cols[k, b]] for k in range(K)], axis=0)
                acc[b, :, LANES[n]] = jnp.dot(left, right, preferred_element_type=F32)

        if h < HOPS - 1:
            local_hub = pick(acc)
        for d in FAR_FIRST[::-1]:
            src, landed = arrival(h, d)
            landed.wait_recv()
            third_copy(h, src, core).start()

        @pl.loop(0, NG)
        def _(src):
            third_copy(h, src, 1 - core).wait_recv()

        if h == HOPS - 1:
            break

        gathered = gbufs[h][...].reshape(HUBS, WIDTH)
        y = local_hub + jnp.dot(hub_w, gathered, preferred_element_type=F32)[:2]
        x = times(y, hub_scale).astype(BF16)
        send_first(h + 1, times(x.astype(F32), hub_scale).astype(BF16))

        for n, (at, count) in enumerate(CHUNKS):
            picked = [(j, s, *listed(j, s, count)) for j in range(2) for s in range(2)]
            prod = jnp.dot(
                jnp.concatenate([wv[b] for _, _, b, _ in picked], axis=0),
                gbufs[h][:, :, :, LANES[n]].reshape(HUBS, count), preferred_element_type=F32)
            for i, (j, s, b, live) in enumerate(picked):
                scale = inv[b]
                x = times(acc[b, :, LANES[n]] + prod[i * TILE : (i + 1) * TILE], scale).astype(BF16)
                halo[h + 1, j, s, :, LANES[n]] = jnp.where(live, times(x.astype(F32), scale), 0.0).astype(BF16)
            send_halo(h + 1, n)

        for n, (first, count) in enumerate(CHUNKS):
            hub_part = gbufs[h][:, :, :, LANES[n]].reshape(HUBS, count)

            @pl.loop(0, 2)
            def _(half):
                w_rows = wv[pl.ds(half * 4, 4)].reshape(4 * TILE, HUBS)
                prod = jnp.dot(w_rows, hub_part, preferred_element_type=F32)
                for q in range(4):
                    b = half * 4 + q
                    scale = inv[b]
                    for j in range(count // TILE):
                        at = slice(first + j * TILE, first + (j + 1) * TILE)
                        y = acc[b, :, at] + prod[q * TILE : (q + 1) * TILE, j * TILE : (j + 1) * TILE]
                        x = (y * scale).astype(BF16)
                        xo[h, b, :, at] = x
                        exts[h + 1][n][b, :, j * TILE : (j + 1) * TILE] = (x.astype(F32) * scale).astype(BF16)

    for h in range(HOPS):
        @pl.loop(0, NZ)
        def _(d):
            q, copy = first_copy(h, d)

            @pl.when(q != me)
            def _():
                copy.wait_send()

        @pl.loop(1, NG)
        def _(d):
            second_copy(h, d).wait_send()

        @pl.loop(0, NG)
        def _(src):
            third_copy(h, src, core).wait_send()

        for n in range(len(CHUNKS)):
            @pl.when(me > 0)
            def _():
                to_left(h, n).wait_send()

            @pl.when(me < N_DOM - 1)
            def _():
                to_right(h, n).wait_send()


def last(xo, wv, inv, acc, gbuf, outf, oute, x3, sem):
    def put(h, src, first, count, i):
        if first < F:
            dst = outf.at[h, :, :, first : first + count]
        else:
            dst = oute.at[h]
        return pltpu.make_async_copy(src, dst, sem.at[i])

    puts = [put(h, xo.at[h, :, :, first : first + count], first, count, 2 * h + (first > 0))
            for h in range(HOPS - 1) for first, count in ((0, F), (F, E))]
    for p in puts:
        p.start()
    for n, (first, count) in enumerate(CHUNKS):
        lanes = slice(first, first + count)
        hub_part = gbuf[:, :, :, lanes].reshape(HUBS, count)

        @pl.loop(0, 2)
        def _(half):
            w_rows = wv[pl.ds(half * 4, 4)].reshape(4 * TILE, HUBS)
            prod = jnp.dot(w_rows, hub_part, preferred_element_type=F32)
            for q in range(4):
                b = half * 4 + q
                scale = inv[b]
                for j in range(count // TILE):
                    at = slice(first + j * TILE, first + (j + 1) * TILE)
                    y = acc[b, :, at] + prod[q * TILE : (q + 1) * TILE, j * TILE : (j + 1) * TILE]
                    x3[b, :, at] = (y * scale).astype(BF16)

        p = put(HOPS - 1, x3.at[:, :, lanes], first, count, 4 + n)
        p.start()
        puts.append(p)
    for p in puts:
        p.wait()


def body(features, embeddings, tile_values, tile_columns, send_blocks, send_count, hub_rows, hub_weight, degree):
    hbm = pl.BlockSpec(memory_space=pltpu.HBM)
    vmem = pl.BlockSpec(memory_space=pltpu.VMEM)
    dma = pltpu.SemaphoreType.DMA
    outs = [
        ((HOPS - 1, BLOCKS, TILE, WIDTH), BF16),
        ((BLOCKS, TILE, HUBS), BF16),
        ((BLOCKS, TILE, TILE), F32),
        ((BLOCKS, TILE, WIDTH), F32),
        ((NG, 2, 16, WIDTH), BF16),
    ]
    held = pl.pallas_call(
        kernel,
        out_shape=[pltpu.VMEM(*o) for o in outs],
        in_specs=[hbm] * 9,
        out_specs=[vmem] * 5,
        scratch_shapes=[
            pltpu.VMEM((8, 128), jnp.int32),
            pltpu.SMEM((K, BLOCKS), jnp.int32),
            pltpu.SMEM((1, 2, 2), jnp.int32),
            pltpu.SMEM((1, 2), jnp.int32),
            pltpu.SMEM((2,), jnp.int32),
            pltpu.VMEM((BLOCKS, TILE, F), BF16),
            pltpu.VMEM((BLOCKS, TILE, E), BF16),
            pltpu.VMEM((BLOCKS, K, TILE, TILE), BF16),
            *[pltpu.VMEM((12, TILE, count), BF16) for _ in range(HOPS) for _, count in CHUNKS],
            pltpu.VMEM((HOPS, 2, 2, TILE, WIDTH), BF16),
            pltpu.VMEM((HOPS, 2, WIDTH), BF16),
            pltpu.VMEM((HOPS, NZ, 2, WIDTH), BF16),
            pltpu.VMEM((HOPS, 16, WIDTH), BF16),
            pltpu.VMEM((NG, 2, 16, WIDTH), BF16),
            pltpu.VMEM((NG, 2, 16, WIDTH), BF16),
            dma((9,)),
            dma((HOPS, 2, len(CHUNKS))),
            dma((HOPS, 2, len(CHUNKS))),
            dma((HOPS, NZ)),
            dma((HOPS, NZ)),
            dma((HOPS, NG)),
            dma((HOPS, NG)),
            dma((HOPS, NG)),
            dma((HOPS, NG)),
        ],
        compiler_params=pltpu.CompilerParams(
            collective_id=0, has_side_effects=True, vmem_limit_bytes=59_000_000
        ),
        name="hops",
    )(
        features.reshape(BLOCKS, TILE, F), embeddings.reshape(BLOCKS, TILE, E), tile_values,
        hub_weight.reshape(BLOCKS, TILE, HUBS), degree.reshape(8, 128), tile_columns.T,
        send_blocks, send_count, hub_rows,
    )
    outf, oute = pl.pallas_call(
        last,
        out_shape=(
            jax.ShapeDtypeStruct((HOPS, BLOCKS, TILE, F), BF16),
            jax.ShapeDtypeStruct((HOPS, BLOCKS, TILE, E), BF16),
        ),
        in_specs=[vmem] * 5,
        out_specs=(hbm, hbm),
        scratch_shapes=[pltpu.VMEM((BLOCKS, TILE, WIDTH), BF16), dma((7,))],
        compiler_params=pltpu.CompilerParams(vmem_limit_bytes=16 * 1024 * 1024),
        name="last",
    )(*held)
    return outf.reshape(HOPS, ROWS, F), oute.reshape(HOPS, ROWS, E)


def solution(mesh):
    dom = P("dom", None)
    placed = (dom, dom, P("dom", None, None, None), dom, P("dom", None, None), dom, P("dom"), dom, P("dom"))
    return jax.shard_map(
        body,
        mesh=mesh,
        in_specs=placed,
        out_specs=(P(None, "dom", None), P(None, "dom", None)),
        check_vma=False,
    )
```

```python
import jax
import jax.numpy as jnp
from jax import lax
from jax.experimental import pallas as pl
from jax.experimental.pallas import tpu as pltpu
from jax.sharding import PartitionSpec as P

HOPS = 3
NX, NY, NZ = 4, 4, 8
NG = NX * NY
N_DOM = NG * NZ * 2
HALF_Z = NZ // 2
TILE = 128
ROWS = 1024
BLOCKS = 8
K = 4
F, E = 512, 128
WIDTH = F + E
HUBS = 512
CHUNKS = ((0, 256), (256, 256), (512, 128))
LANES = tuple(slice(first, first + count) for first, count in CHUNKS)
FAR_FIRST = (10, 6, 9, 11, 14, 2, 8, 5, 7, 13, 15, 1, 3, 4, 12)
RING_FAR_FIRST = (4, 3, 5, 2, 6, 1, 7, 0)
BF16, F32 = jnp.bfloat16, jnp.float32


def kernel(
    feat, emb, tv_hbm, w_hbm, deg_hbm, cols_hbm, sblk_hbm, scnt_hbm, hubs_hbm,
    xo, wv, inv, acc, gbuf2,
    deg, cols, sblk, scnt, hubs, xf, xe, tv, e00, e01, e02, e10, e11, e12, e20, e21, e22, halo, hsend, land, tsend, gbuf0, gbuf1,
    in_sem, hs_sem, hr_sem, s1, r1, s2, r2, s3, r3,
):
    exts = ((e00, e01, e02), (e10, e11, e12), (e20, e21, e22))
    gbufs = (gbuf0, gbuf1, gbuf2)
    me = lax.axis_index("dom")
    core = lax.rem(me, 2)
    z = lax.rem(lax.div(me, 2), NZ)
    g = lax.div(me, 2 * NZ)
    gx = lax.div(g, NY)
    gy = lax.rem(g, NY)
    partner = me + 1 - 2 * core
    cls = lax.div(z, HALF_Z)
    own_slot = lax.rem(z, HALF_Z) * 2 + core

    def dev(g_, z_, c_):
        return (g_ * NZ + z_) * 2 + c_

    def plane(d):
        x_ = lax.rem(gx + lax.div(d, NY), NX)
        y_ = lax.rem(gy + lax.rem(d, NY), NY)
        return x_ * NY + y_

    def remote(src, dst, send, recv, q):
        return pltpu.make_async_remote_copy(
            src_ref=src, dst_ref=dst, send_sem=send, recv_sem=recv,
            device_id={"dom": q}, device_id_type=pl.DeviceIdType.MESH)

    def first_copy(h, d):
        q = dev(g, lax.rem(z + d, NZ), cls)
        return q, remote(hsend.at[h], land.at[h, own_slot], s1.at[h, d], r1.at[h, own_slot], q)

    def second_copy(h, d):
        return remote(tsend.at[h], gbufs[h].at[g, core], s2.at[h, d], r2.at[h, g], dev(plane(d), z, core))

    def arrival(h, d):
        src = plane(d)
        return src, remote(tsend.at[h], gbufs[h].at[src, core], s2.at[h, d], r2.at[h, src], dev(src, z, core))

    def third_copy(h, src, lane):
        return remote(gbufs[h].at[src, lane], gbufs[h].at[src, lane], s3.at[h, src], r3.at[h, src], partner)

    def to_left(h, n):
        return remote(halo.at[h, 0, :, :, LANES[n]], exts[h][n].at[10:12], hs_sem.at[h, 0, n], hr_sem.at[h, 0, n], me - 1)

    def to_right(h, n):
        return remote(halo.at[h, 1, :, :, LANES[n]], exts[h][n].at[8:10], hs_sem.at[h, 1, n], hr_sem.at[h, 1, n], me + 1)

    small = [
        pltpu.make_async_copy(src, dst, in_sem.at[4 + i])
        for i, (src, dst) in enumerate(
            ((deg_hbm, deg), (cols_hbm, cols), (sblk_hbm, sblk), (scnt_hbm, scnt), (hubs_hbm, hubs)))
    ]
    loads = [
        pltpu.make_async_copy(feat, xf, in_sem.at[0]),
        pltpu.make_async_copy(emb, xe, in_sem.at[1]),
        pltpu.make_async_copy(w_hbm, wv, in_sem.at[2]),
        pltpu.make_async_copy(tv_hbm, tv, in_sem.at[3]),
    ]
    for load in small + loads:
        load.start()

    barrier = pltpu.get_barrier_semaphore()

    @pl.loop(1, 2 * NZ)
    def _(d):
        pl.semaphore_signal(barrier, inc=1, device_id={"dom": g * 2 * NZ + lax.rem(z * 2 + core + d, 2 * NZ)})

    @pl.loop(1, NG)
    def _(d):
        pl.semaphore_signal(barrier, inc=1, device_id={"dom": dev(plane(d), z, core)})

    @pl.when(me > 0)
    def _():
        pl.semaphore_signal(barrier, inc=1, device_id={"dom": me - 1})

    @pl.when(me < N_DOM - 1)
    def _():
        pl.semaphore_signal(barrier, inc=1, device_id={"dom": me + 1})

    def barrier_wait():
        extra = jnp.where(me > 0, 1, 0) + jnp.where(me < N_DOM - 1, 1, 0)
        pl.semaphore_wait(barrier, 2 * NZ - 1 + NG - 1 + extra)

    for load in small:
        load.wait()
    root = lax.rsqrt(deg[...].astype(F32))
    for b in range(BLOCKS):
        inv[b] = jnp.broadcast_to(root[b : b + 1, :], (TILE, TILE)).T

    @pl.when(me == 0)
    def _():
        for h in range(HOPS):
            for n, (_, count) in enumerate(CHUNKS):
                exts[h][n][8:10] = jnp.zeros((2, TILE, count), BF16)

    @pl.when(me == N_DOM - 1)
    def _():
        for h in range(HOPS):
            for n, (_, count) in enumerate(CHUNKS):
                exts[h][n][10:12] = jnp.zeros((2, TILE, count), BF16)

    hub_block = [lax.shift_right_logical(hubs[i], 7) for i in range(2)]
    hub_in = [jnp.bitwise_and(hubs[i], TILE - 1) for i in range(2)]

    def pick(ref):
        rows = []
        for i in range(2):
            block = ref[hub_block[i]].astype(F32)
            hit = lax.broadcasted_iota(jnp.int32, block.shape, 0) == hub_in[i]
            rows.append(jnp.sum(jnp.where(hit, block, 0.0), axis=0, keepdims=True))
        return jnp.concatenate(rows, axis=0)

    def times(block, scale):
        width = block.shape[-1]
        return jnp.concatenate([block[:, j : j + TILE] * scale for j in range(0, width, TILE)], axis=1)

    def send_first(h, pair):
        hsend[h] = pair
        if h == 0:
            barrier_wait()

        for d in RING_FAR_FIRST:
            q, copy = first_copy(h, d)

            @pl.when(q != me)
            def _():
                copy.start()

        @pl.when(cls == core)
        def _():
            land[h, own_slot] = pair

    def listed(j, s, width):
        live = lax.broadcasted_iota(jnp.int32, (TILE, width), 0) * 0 + s < scnt[0, j]
        return sblk[0, j, s], live

    def send_halo(h, n):
        @pl.when(me > 0)
        def _():
            to_left(h, n).start()

        @pl.when(me < N_DOM - 1)
        def _():
            to_right(h, n).start()

    hub_scale = pick(inv)
    loads[0].wait()
    loads[1].wait()
    first = jnp.concatenate([pick(xf), pick(xe)], axis=1)
    send_first(0, times(first, hub_scale).astype(BF16))
    for n, (at, count) in enumerate(CHUNKS):
        for j in range(2):
            for s in range(2):
                b, live = listed(j, s, count)
                block = xf[b, :, LANES[n]] if at < F else xe[b]
                halo[0, j, s, :, LANES[n]] = jnp.where(live, times(block.astype(F32), inv[b]), 0.0).astype(BF16)
        send_halo(0, n)

    @pl.loop(0, BLOCKS)
    def _(b):
        scale = inv[b]
        for n, (at, count) in enumerate(CHUNKS):
            block = xf[b, :, LANES[n]] if at < F else xe[b]
            exts[0][n][b] = times(block.astype(F32), scale).astype(BF16)

    loads[2].wait()
    loads[3].wait()
    hub_w = jnp.concatenate([pick(wv), jnp.zeros((14, HUBS), F32)], axis=0).astype(BF16)

    for h in range(HOPS):
        for s in range(NZ):
            source = dev(g, core * HALF_Z + s // 2, s % 2)

            @pl.when(source != me)
            def _():
                remote(hsend.at[h], land.at[h, s], s1.at[h, s], r1.at[h, s], source).wait_recv()

        whole = jnp.concatenate([land[h, s].astype(F32) for s in range(NZ)], axis=0).astype(BF16)
        tsend[h] = whole
        gbufs[h][g, core] = whole

        for d in FAR_FIRST:
            second_copy(h, d).start()
        third_copy(h, g, core).start()

        for n, (at, count) in enumerate(CHUNKS):
            @pl.when(me > 0)
            def _():
                to_right(h, n).wait_recv()

            @pl.when(me < N_DOM - 1)
            def _():
                to_left(h, n).wait_recv()

            @pl.loop(0, BLOCKS, unroll=8)
            def _(b):
                left = jnp.concatenate([tv[b, k] for k in range(K)], axis=1)
                right = jnp.concatenate([exts[h][n][cols[k, b]] for k in range(K)], axis=0)
                acc[b, :, LANES[n]] = jnp.dot(left, right, preferred_element_type=F32)

        if h < HOPS - 1:
            local_hub = pick(acc)
        for d in FAR_FIRST[::-1]:
            src, landed = arrival(h, d)
            landed.wait_recv()
            third_copy(h, src, core).start()

        @pl.loop(0, NG)
        def _(src):
            third_copy(h, src, 1 - core).wait_recv()

        if h == HOPS - 1:
            break

        gathered = gbufs[h][...].reshape(HUBS, WIDTH)
        y = local_hub + jnp.dot(hub_w, gathered, preferred_element_type=F32)[:2]
        x = times(y, hub_scale).astype(BF16)
        send_first(h + 1, times(x.astype(F32), hub_scale).astype(BF16))

        for n, (at, count) in enumerate(CHUNKS):
            picked = [(j, s, *listed(j, s, count)) for j in range(2) for s in range(2)]
            prod = jnp.dot(
                jnp.concatenate([wv[b] for _, _, b, _ in picked], axis=0),
                gbufs[h][:, :, :, LANES[n]].reshape(HUBS, count), preferred_element_type=F32)
            for i, (j, s, b, live) in enumerate(picked):
                scale = inv[b]
                x = times(acc[b, :, LANES[n]] + prod[i * TILE : (i + 1) * TILE], scale).astype(BF16)
                halo[h + 1, j, s, :, LANES[n]] = jnp.where(live, times(x.astype(F32), scale), 0.0).astype(BF16)
            send_halo(h + 1, n)

        for n, (first, count) in enumerate(CHUNKS):
            hub_part = gbufs[h][:, :, :, LANES[n]].reshape(HUBS, count)

            @pl.loop(0, 2, unroll=2)
            def _(half):
                w_rows = wv[pl.ds(half * 4, 4)].reshape(4 * TILE, HUBS)
                prod = jnp.dot(w_rows, hub_part, preferred_element_type=F32)
                for q in range(4):
                    b = half * 4 + q
                    scale = inv[b]
                    for j in range(count // TILE):
                        at = slice(first + j * TILE, first + (j + 1) * TILE)
                        y = acc[b, :, at] + prod[q * TILE : (q + 1) * TILE, j * TILE : (j + 1) * TILE]
                        x = (y * scale).astype(BF16)
                        xo[h, b, :, at] = x
                        exts[h + 1][n][b, :, j * TILE : (j + 1) * TILE] = (x.astype(F32) * scale).astype(BF16)

    for h in range(HOPS):
        @pl.loop(0, NZ)
        def _(d):
            q, copy = first_copy(h, d)

            @pl.when(q != me)
            def _():
                copy.wait_send()

        @pl.loop(1, NG)
        def _(d):
            second_copy(h, d).wait_send()

        @pl.loop(0, NG)
        def _(src):
            third_copy(h, src, core).wait_send()

        for n in range(len(CHUNKS)):
            @pl.when(me > 0)
            def _():
                to_left(h, n).wait_send()

            @pl.when(me < N_DOM - 1)
            def _():
                to_right(h, n).wait_send()


def last(xo, wv, inv, acc, gbuf, outf, oute, x3, sem):
    def put(h, src, first, count, i):
        if first < F:
            dst = outf.at[h, :, :, first : first + count]
        else:
            dst = oute.at[h]
        return pltpu.make_async_copy(src, dst, sem.at[i])

    puts = [put(h, xo.at[h, :, :, first : first + count], first, count, 2 * h + (first > 0))
            for h in range(HOPS - 1) for first, count in ((0, F), (F, E))]
    for p in puts:
        p.start()
    for n, (first, count) in enumerate(CHUNKS):
        lanes = slice(first, first + count)
        hub_part = gbuf[:, :, :, lanes].reshape(HUBS, count)

        @pl.loop(0, 2)
        def _(half):
            w_rows = wv[pl.ds(half * 4, 4)].reshape(4 * TILE, HUBS)
            prod = jnp.dot(w_rows, hub_part, preferred_element_type=F32)
            for q in range(4):
                b = half * 4 + q
                scale = inv[b]
                for j in range(count // TILE):
                    at = slice(first + j * TILE, first + (j + 1) * TILE)
                    y = acc[b, :, at] + prod[q * TILE : (q + 1) * TILE, j * TILE : (j + 1) * TILE]
                    x3[b, :, at] = (y * scale).astype(BF16)

        p = put(HOPS - 1, x3.at[:, :, lanes], first, count, 4 + n)
        p.start()
        puts.append(p)
    for p in puts:
        p.wait()


def body(features, embeddings, tile_values, tile_columns, send_blocks, send_count, hub_rows, hub_weight, degree):
    hbm = pl.BlockSpec(memory_space=pltpu.HBM)
    vmem = pl.BlockSpec(memory_space=pltpu.VMEM)
    dma = pltpu.SemaphoreType.DMA
    outs = [
        ((HOPS - 1, BLOCKS, TILE, WIDTH), BF16),
        ((BLOCKS, TILE, HUBS), BF16),
        ((BLOCKS, TILE, TILE), F32),
        ((BLOCKS, TILE, WIDTH), F32),
        ((NG, 2, 16, WIDTH), BF16),
    ]
    held = pl.pallas_call(
        kernel,
        out_shape=[pltpu.VMEM(*o) for o in outs],
        in_specs=[hbm] * 9,
        out_specs=[vmem] * 5,
        scratch_shapes=[
            pltpu.VMEM((8, 128), jnp.int32),
            pltpu.SMEM((K, BLOCKS), jnp.int32),
            pltpu.SMEM((1, 2, 2), jnp.int32),
            pltpu.SMEM((1, 2), jnp.int32),
            pltpu.SMEM((2,), jnp.int32),
            pltpu.VMEM((BLOCKS, TILE, F), BF16),
            pltpu.VMEM((BLOCKS, TILE, E), BF16),
            pltpu.VMEM((BLOCKS, K, TILE, TILE), BF16),
            *[pltpu.VMEM((12, TILE, count), BF16) for _ in range(HOPS) for _, count in CHUNKS],
            pltpu.VMEM((HOPS, 2, 2, TILE, WIDTH), BF16),
            pltpu.VMEM((HOPS, 2, WIDTH), BF16),
            pltpu.VMEM((HOPS, NZ, 2, WIDTH), BF16),
            pltpu.VMEM((HOPS, 16, WIDTH), BF16),
            pltpu.VMEM((NG, 2, 16, WIDTH), BF16),
            pltpu.VMEM((NG, 2, 16, WIDTH), BF16),
            dma((9,)),
            dma((HOPS, 2, len(CHUNKS))),
            dma((HOPS, 2, len(CHUNKS))),
            dma((HOPS, NZ)),
            dma((HOPS, NZ)),
            dma((HOPS, NG)),
            dma((HOPS, NG)),
            dma((HOPS, NG)),
            dma((HOPS, NG)),
        ],
        compiler_params=pltpu.CompilerParams(
            collective_id=0, has_side_effects=True, vmem_limit_bytes=59_000_000
        ),
        name="hops",
    )(
        features.reshape(BLOCKS, TILE, F), embeddings.reshape(BLOCKS, TILE, E), tile_values,
        hub_weight.reshape(BLOCKS, TILE, HUBS), degree.reshape(8, 128), tile_columns.T,
        send_blocks, send_count, hub_rows,
    )
    outf, oute = pl.pallas_call(
        last,
        out_shape=(
            jax.ShapeDtypeStruct((HOPS, BLOCKS, TILE, F), BF16),
            jax.ShapeDtypeStruct((HOPS, BLOCKS, TILE, E), BF16),
        ),
        in_specs=[vmem] * 5,
        out_specs=(hbm, hbm),
        scratch_shapes=[pltpu.VMEM((BLOCKS, TILE, WIDTH), BF16), dma((7,))],
        compiler_params=pltpu.CompilerParams(vmem_limit_bytes=16 * 1024 * 1024),
        name="last",
    )(*held)
    return outf.reshape(HOPS, ROWS, F), oute.reshape(HOPS, ROWS, E)


def solution(mesh):
    dom = P("dom", None)
    placed = (dom, dom, P("dom", None, None, None), dom, P("dom", None, None), dom, P("dom"), dom, P("dom"))
    return jax.shard_map(
        body,
        mesh=mesh,
        in_specs=placed,
        out_specs=(P(None, "dom", None), P(None, "dom", None)),
        check_vma=False,
    )
```

```python
import jax
import jax.numpy as jnp
from jax import lax
from jax.experimental import pallas as pl
from jax.experimental.pallas import tpu as pltpu
from jax.sharding import PartitionSpec as P

HOPS = 3
NX, NY, NZ = 4, 4, 8
NG = NX * NY
N_DOM = NG * NZ * 2
HALF_Z = NZ // 2
TILE = 128
ROWS = 1024
BLOCKS = 8
K = 4
F, E = 512, 128
WIDTH = F + E
HUBS = 512
CHUNKS = ((0, 256), (256, 256), (512, 128))
LANES = tuple(slice(first, first + count) for first, count in CHUNKS)
FAR_FIRST = (10, 6, 9, 11, 14, 2, 8, 5, 7, 13, 15, 1, 3, 4, 12)
RING_FAR_FIRST = (4, 3, 5, 2, 6, 1, 7, 0)
BF16, F32 = jnp.bfloat16, jnp.float32


def kernel(
    feat, emb, tv_hbm, w_hbm, deg_hbm, cols_hbm, sblk_hbm, scnt_hbm, hubs_hbm,
    xo, wv, inv, acc, gbuf2,
    deg, cols, sblk, scnt, hubs, xf, xe, tv, e00, e01, e02, e10, e11, e12, e20, e21, e22, halo, hsend, land, tsend, gbuf0, gbuf1,
    in_sem, hs_sem, hr_sem, s1, r1, s2, r2, s3, r3,
):
    exts = ((e00, e01, e02), (e10, e11, e12), (e20, e21, e22))
    gbufs = (gbuf0, gbuf1, gbuf2)
    me = lax.axis_index("dom")
    core = lax.rem(me, 2)
    z = lax.rem(lax.div(me, 2), NZ)
    g = lax.div(me, 2 * NZ)
    gx = lax.div(g, NY)
    gy = lax.rem(g, NY)
    partner = me + 1 - 2 * core
    cls = lax.div(z, HALF_Z)
    own_slot = lax.rem(z, HALF_Z) * 2 + core

    def dev(g_, z_, c_):
        return (g_ * NZ + z_) * 2 + c_

    def plane(d):
        x_ = lax.rem(gx + lax.div(d, NY), NX)
        y_ = lax.rem(gy + lax.rem(d, NY), NY)
        return x_ * NY + y_

    def target(d):
        way = 1 - 2 * core
        x_ = lax.rem(gx + NX + way * (d // NY), NX)
        y_ = lax.rem(gy + NY + way * (d % NY), NY)
        return x_ * NY + y_

    def remote(src, dst, send, recv, q):
        return pltpu.make_async_remote_copy(
            src_ref=src, dst_ref=dst, send_sem=send, recv_sem=recv,
            device_id={"dom": q}, device_id_type=pl.DeviceIdType.MESH)

    def first_copy(h, d):
        q = dev(g, lax.rem(z + d, NZ), cls)
        return q, remote(hsend.at[h], land.at[h, own_slot], s1.at[h, d], r1.at[h, own_slot], q)

    def second_copy(h, d):
        return remote(tsend.at[h], gbufs[h].at[g, core], s2.at[h, d], r2.at[h, g], dev(target(d), z, core))

    def arrival(h, d):
        src = plane(d)
        return src, remote(tsend.at[h], gbufs[h].at[src, core], s2.at[h, d], r2.at[h, src], dev(src, z, core))

    def third_copy(h, src, lane):
        return remote(gbufs[h].at[src, lane], gbufs[h].at[src, lane], s3.at[h, src], r3.at[h, src], partner)

    def to_left(h, n):
        return remote(halo.at[h, 0, :, :, LANES[n]], exts[h][n].at[10:12], hs_sem.at[h, 0, n], hr_sem.at[h, 0, n], me - 1)

    def to_right(h, n):
        return remote(halo.at[h, 1, :, :, LANES[n]], exts[h][n].at[8:10], hs_sem.at[h, 1, n], hr_sem.at[h, 1, n], me + 1)

    small = [
        pltpu.make_async_copy(src, dst, in_sem.at[4 + i])
        for i, (src, dst) in enumerate(
            ((deg_hbm, deg), (cols_hbm, cols), (sblk_hbm, sblk), (scnt_hbm, scnt), (hubs_hbm, hubs)))
    ]
    loads = [
        pltpu.make_async_copy(feat, xf, in_sem.at[0]),
        pltpu.make_async_copy(emb, xe, in_sem.at[1]),
        pltpu.make_async_copy(w_hbm, wv, in_sem.at[2]),
        pltpu.make_async_copy(tv_hbm, tv, in_sem.at[3]),
    ]
    barrier = pltpu.get_barrier_semaphore()

    @pl.loop(1, 2 * NZ)
    def _(d):
        pl.semaphore_signal(barrier, inc=1, device_id={"dom": g * 2 * NZ + lax.rem(z * 2 + core + d, 2 * NZ)})

    @pl.loop(1, NG)
    def _(d):
        pl.semaphore_signal(barrier, inc=1, device_id={"dom": dev(plane(d), z, core)})

    @pl.when(me > 0)
    def _():
        pl.semaphore_signal(barrier, inc=1, device_id={"dom": me - 1})

    @pl.when(me < N_DOM - 1)
    def _():
        pl.semaphore_signal(barrier, inc=1, device_id={"dom": me + 1})

    for load in small + loads:
        load.start()

    def barrier_wait():
        extra = jnp.where(me > 0, 1, 0) + jnp.where(me < N_DOM - 1, 1, 0)
        pl.semaphore_wait(barrier, 2 * NZ - 1 + NG - 1 + extra)

    for load in small:
        load.wait()
    root = lax.rsqrt(deg[...].astype(F32))
    for b in range(BLOCKS):
        inv[b] = jnp.broadcast_to(root[b : b + 1, :], (TILE, TILE)).T

    @pl.when(me == 0)
    def _():
        for h in range(HOPS):
            for n, (_, count) in enumerate(CHUNKS):
                exts[h][n][8:10] = jnp.zeros((2, TILE, count), BF16)

    @pl.when(me == N_DOM - 1)
    def _():
        for h in range(HOPS):
            for n, (_, count) in enumerate(CHUNKS):
                exts[h][n][10:12] = jnp.zeros((2, TILE, count), BF16)

    hub_block = [lax.shift_right_logical(hubs[i], 7) for i in range(2)]
    hub_in = [jnp.bitwise_and(hubs[i], TILE - 1) for i in range(2)]

    def pick(ref):
        rows = []
        for i in range(2):
            block = ref[hub_block[i]].astype(F32)
            hit = lax.broadcasted_iota(jnp.int32, block.shape, 0) == hub_in[i]
            rows.append(jnp.sum(jnp.where(hit, block, 0.0), axis=0, keepdims=True))
        return jnp.concatenate(rows, axis=0)

    def times(block, scale):
        width = block.shape[-1]
        return jnp.concatenate([block[:, j : j + TILE] * scale for j in range(0, width, TILE)], axis=1)

    def send_first(h, pair):
        hsend[h] = pair
        if h == 0:
            barrier_wait()

        for d in RING_FAR_FIRST:
            q, copy = first_copy(h, d)

            @pl.when(q != me)
            def _():
                copy.start()

        @pl.when(cls == core)
        def _():
            land[h, own_slot] = pair

    def listed(j, s, width):
        live = lax.broadcasted_iota(jnp.int32, (TILE, width), 0) * 0 + s < scnt[0, j]
        return sblk[0, j, s], live

    def send_halo(h, n):
        @pl.when(me > 0)
        def _():
            to_left(h, n).start()

        @pl.when(me < N_DOM - 1)
        def _():
            to_right(h, n).start()

    hub_scale = pick(inv)
    loads[0].wait()
    loads[1].wait()
    first = jnp.concatenate([pick(xf), pick(xe)], axis=1)
    send_first(0, times(first, hub_scale).astype(BF16))
    for n, (at, count) in enumerate(CHUNKS):
        for j in range(2):
            for s in range(2):
                b, live = listed(j, s, count)
                block = xf[b, :, LANES[n]] if at < F else xe[b]
                halo[0, j, s, :, LANES[n]] = jnp.where(live, times(block.astype(F32), inv[b]), 0.0).astype(BF16)
        send_halo(0, n)

    @pl.loop(0, BLOCKS)
    def _(b):
        scale = inv[b]
        for n, (at, count) in enumerate(CHUNKS):
            block = xf[b, :, LANES[n]] if at < F else xe[b]
            exts[0][n][b] = times(block.astype(F32), scale).astype(BF16)

    loads[2].wait()
    loads[3].wait()
    hub_w = jnp.concatenate([pick(wv), jnp.zeros((14, HUBS), F32)], axis=0).astype(BF16)

    for h in range(HOPS):
        for s in range(NZ):
            source = dev(g, core * HALF_Z + s // 2, s % 2)

            @pl.when(source != me)
            def _():
                remote(hsend.at[h], land.at[h, s], s1.at[h, s], r1.at[h, s], source).wait_recv()

        whole = jnp.concatenate([land[h, s].astype(F32) for s in range(NZ)], axis=0).astype(BF16)
        tsend[h] = whole
        gbufs[h][g, core] = whole

        for d in FAR_FIRST:
            second_copy(h, d).start()
        third_copy(h, g, core).start()

        for n, (at, count) in enumerate(CHUNKS):
            @pl.when(me > 0)
            def _():
                to_right(h, n).wait_recv()

            @pl.when(me < N_DOM - 1)
            def _():
                to_left(h, n).wait_recv()

            @pl.loop(0, BLOCKS, unroll=8)
            def _(b):
                left = jnp.concatenate([tv[b, k] for k in range(K)], axis=1)
                right = jnp.concatenate([exts[h][n][cols[k, b]] for k in range(K)], axis=0)
                acc[b, :, LANES[n]] = jnp.dot(left, right, preferred_element_type=F32)

        if h < HOPS - 1:
            local_hub = pick(acc)
        for d in FAR_FIRST[::-1]:
            src, landed = arrival(h, d)
            landed.wait_recv()
            third_copy(h, src, core).start()

        @pl.loop(0, NG)
        def _(src):
            third_copy(h, src, 1 - core).wait_recv()

        if h == HOPS - 1:
            break

        gathered = gbufs[h][...].reshape(HUBS, WIDTH)
        y = local_hub + jnp.dot(hub_w, gathered, preferred_element_type=F32)[:2]
        x = times(y, hub_scale).astype(BF16)
        send_first(h + 1, times(x.astype(F32), hub_scale).astype(BF16))

        for n, (at, count) in enumerate(CHUNKS):
            picked = [(j, s, *listed(j, s, count)) for j in range(2) for s in range(2)]
            prod = jnp.dot(
                jnp.concatenate([wv[b] for _, _, b, _ in picked], axis=0),
                gbufs[h][:, :, :, LANES[n]].reshape(HUBS, count), preferred_element_type=F32)
            for i, (j, s, b, live) in enumerate(picked):
                scale = inv[b]
                x = times(acc[b, :, LANES[n]] + prod[i * TILE : (i + 1) * TILE], scale).astype(BF16)
                halo[h + 1, j, s, :, LANES[n]] = jnp.where(live, times(x.astype(F32), scale), 0.0).astype(BF16)
            send_halo(h + 1, n)

        for n, (first, count) in enumerate(CHUNKS):
            hub_part = gbufs[h][:, :, :, LANES[n]].reshape(HUBS, count)

            @pl.loop(0, 2, unroll=2)
            def _(half):
                w_rows = wv[pl.ds(half * 4, 4)].reshape(4 * TILE, HUBS)
                prod = jnp.dot(w_rows, hub_part, preferred_element_type=F32)
                for q in range(4):
                    b = half * 4 + q
                    scale = inv[b]
                    for j in range(count // TILE):
                        at = slice(first + j * TILE, first + (j + 1) * TILE)
                        y = acc[b, :, at] + prod[q * TILE : (q + 1) * TILE, j * TILE : (j + 1) * TILE]
                        x = (y * scale).astype(BF16)
                        xo[h, b, :, at] = x
                        exts[h + 1][n][b, :, j * TILE : (j + 1) * TILE] = (x.astype(F32) * scale).astype(BF16)

    for h in range(HOPS):
        @pl.loop(0, NZ)
        def _(d):
            q, copy = first_copy(h, d)

            @pl.when(q != me)
            def _():
                copy.wait_send()

        for d in range(1, NG):
            second_copy(h, d).wait_send()

        @pl.loop(0, NG)
        def _(src):
            third_copy(h, src, core).wait_send()

        for n in range(len(CHUNKS)):
            @pl.when(me > 0)
            def _():
                to_left(h, n).wait_send()

            @pl.when(me < N_DOM - 1)
            def _():
                to_right(h, n).wait_send()


def last(xo, wv, inv, acc, gbuf, outf, oute, x3, sem):
    def put(h, src, first, count, i):
        if first < F:
            dst = outf.at[h, :, :, first : first + count]
        else:
            dst = oute.at[h]
        return pltpu.make_async_copy(src, dst, sem.at[i])

    puts = [put(h, xo.at[h, :, :, first : first + count], first, count, 2 * h + (first > 0))
            for h in range(HOPS - 1) for first, count in ((0, F), (F, E))]
    for p in puts:
        p.start()
    for n, (first, count) in enumerate(CHUNKS):
        lanes = slice(first, first + count)
        hub_part = gbuf[:, :, :, lanes].reshape(HUBS, count)

        @pl.loop(0, 2, unroll=2)
        def _(half):
            w_rows = wv[pl.ds(half * 4, 4)].reshape(4 * TILE, HUBS)
            prod = jnp.dot(w_rows, hub_part, preferred_element_type=F32)
            for q in range(4):
                b = half * 4 + q
                scale = inv[b]
                for j in range(count // TILE):
                    at = slice(first + j * TILE, first + (j + 1) * TILE)
                    y = acc[b, :, at] + prod[q * TILE : (q + 1) * TILE, j * TILE : (j + 1) * TILE]
                    x3[b, :, at] = (y * scale).astype(BF16)

        p = put(HOPS - 1, x3.at[:, :, lanes], first, count, 4 + n)
        p.start()
        puts.append(p)
    for p in puts:
        p.wait()


def body(features, embeddings, tile_values, tile_columns, send_blocks, send_count, hub_rows, hub_weight, degree):
    hbm = pl.BlockSpec(memory_space=pltpu.HBM)
    vmem = pl.BlockSpec(memory_space=pltpu.VMEM)
    dma = pltpu.SemaphoreType.DMA
    outs = [
        ((HOPS - 1, BLOCKS, TILE, WIDTH), BF16),
        ((BLOCKS, TILE, HUBS), BF16),
        ((BLOCKS, TILE, TILE), F32),
        ((BLOCKS, TILE, WIDTH), F32),
        ((NG, 2, 16, WIDTH), BF16),
    ]
    held = pl.pallas_call(
        kernel,
        out_shape=[pltpu.VMEM(*o) for o in outs],
        in_specs=[hbm] * 9,
        out_specs=[vmem] * 5,
        scratch_shapes=[
            pltpu.VMEM((8, 128), jnp.int32),
            pltpu.SMEM((K, BLOCKS), jnp.int32),
            pltpu.SMEM((1, 2, 2), jnp.int32),
            pltpu.SMEM((1, 2), jnp.int32),
            pltpu.SMEM((2,), jnp.int32),
            pltpu.VMEM((BLOCKS, TILE, F), BF16),
            pltpu.VMEM((BLOCKS, TILE, E), BF16),
            pltpu.VMEM((BLOCKS, K, TILE, TILE), BF16),
            *[pltpu.VMEM((12, TILE, count), BF16) for _ in range(HOPS) for _, count in CHUNKS],
            pltpu.VMEM((HOPS, 2, 2, TILE, WIDTH), BF16),
            pltpu.VMEM((HOPS, 2, WIDTH), BF16),
            pltpu.VMEM((HOPS, NZ, 2, WIDTH), BF16),
            pltpu.VMEM((HOPS, 16, WIDTH), BF16),
            pltpu.VMEM((NG, 2, 16, WIDTH), BF16),
            pltpu.VMEM((NG, 2, 16, WIDTH), BF16),
            dma((9,)),
            dma((HOPS, 2, len(CHUNKS))),
            dma((HOPS, 2, len(CHUNKS))),
            dma((HOPS, NZ)),
            dma((HOPS, NZ)),
            dma((HOPS, NG)),
            dma((HOPS, NG)),
            dma((HOPS, NG)),
            dma((HOPS, NG)),
        ],
        compiler_params=pltpu.CompilerParams(
            collective_id=0, has_side_effects=True, vmem_limit_bytes=59_000_000
        ),
        name="hops",
    )(
        features.reshape(BLOCKS, TILE, F), embeddings.reshape(BLOCKS, TILE, E), tile_values,
        hub_weight.reshape(BLOCKS, TILE, HUBS), degree.reshape(8, 128), tile_columns.T,
        send_blocks, send_count, hub_rows,
    )
    outf, oute = pl.pallas_call(
        last,
        out_shape=(
            jax.ShapeDtypeStruct((HOPS, BLOCKS, TILE, F), BF16),
            jax.ShapeDtypeStruct((HOPS, BLOCKS, TILE, E), BF16),
        ),
        in_specs=[vmem] * 5,
        out_specs=(hbm, hbm),
        scratch_shapes=[pltpu.VMEM((BLOCKS, TILE, WIDTH), BF16), dma((7,))],
        compiler_params=pltpu.CompilerParams(vmem_limit_bytes=16 * 1024 * 1024),
        name="last",
    )(*held)
    return outf.reshape(HOPS, ROWS, F), oute.reshape(HOPS, ROWS, E)


def solution(mesh):
    dom = P("dom", None)
    placed = (dom, dom, P("dom", None, None, None), dom, P("dom", None, None), dom, P("dom"), dom, P("dom"))
    return jax.shard_map(
        body,
        mesh=mesh,
        in_specs=placed,
        out_specs=(P(None, "dom", None), P(None, "dom", None)),
        check_vma=False,
    )
```

```python
import jax
import jax.numpy as jnp
from jax import lax
from jax.experimental import pallas as pl
from jax.experimental.pallas import tpu as pltpu
from jax.sharding import PartitionSpec as P

HOPS = 3
NX, NY, NZ = 4, 4, 8
NG = NX * NY
N_DOM = NG * NZ * 2
HALF_Z = NZ // 2
TILE = 128
ROWS = 1024
BLOCKS = 8
K = 4
F, E = 512, 128
WIDTH = F + E
HUBS = 512
CHUNKS = ((0, 256), (256, 256), (512, 128))
LANES = tuple(slice(first, first + count) for first, count in CHUNKS)
FAR_FIRST = (10, 6, 9, 11, 14, 2, 8, 5, 7, 13, 15, 1, 3, 4, 12)
RING_FAR_FIRST = (4, 3, 5, 2, 6, 1, 7, 0)
BF16, F32 = jnp.bfloat16, jnp.float32


def kernel(
    feat, emb, tv_hbm, w_hbm, deg_hbm, cols_hbm, sblk_hbm, scnt_hbm, hubs_hbm,
    xo, wv, inv, acc, gbuf2,
    deg, cols, sblk, scnt, hubs, xf, xe, tv, e00, e01, e02, e10, e11, e12, e20, e21, e22, halo, hsend, land, tsend, gbuf0, gbuf1,
    in_sem, hs_sem, hr_sem, s1, r1, s2, r2, s3, r3,
):
    exts = ((e00, e01, e02), (e10, e11, e12), (e20, e21, e22))
    gbufs = (gbuf0, gbuf1, gbuf2)
    me = lax.axis_index("dom")
    core = lax.rem(me, 2)
    z = lax.rem(lax.div(me, 2), NZ)
    g = lax.div(me, 2 * NZ)
    gx = lax.div(g, NY)
    gy = lax.rem(g, NY)
    partner = me + 1 - 2 * core
    cls = lax.div(z, HALF_Z)
    own_slot = lax.rem(z, HALF_Z) * 2 + core

    def dev(g_, z_, c_):
        return (g_ * NZ + z_) * 2 + c_

    def plane(d):
        x_ = lax.rem(gx + lax.div(d, NY), NX)
        y_ = lax.rem(gy + lax.rem(d, NY), NY)
        return x_ * NY + y_

    def target(d):
        way = 1 - 2 * core
        x_ = lax.rem(gx + NX + way * (d // NY), NX)
        y_ = lax.rem(gy + NY + way * (d % NY), NY)
        return x_ * NY + y_

    def remote(src, dst, send, recv, q):
        return pltpu.make_async_remote_copy(
            src_ref=src, dst_ref=dst, send_sem=send, recv_sem=recv,
            device_id={"dom": q}, device_id_type=pl.DeviceIdType.MESH)

    def first_copy(h, d):
        q = dev(g, lax.rem(z + NZ + (1 - 2 * core) * d, NZ), cls)
        return q, remote(hsend.at[h], land.at[h, own_slot], s1.at[h, d], r1.at[h, own_slot], q)

    def second_copy(h, d):
        return remote(tsend.at[h], gbufs[h].at[g, core], s2.at[h, d], r2.at[h, g], dev(target(d), z, core))

    def arrival(h, d):
        src = plane(d)
        return src, remote(tsend.at[h], gbufs[h].at[src, core], s2.at[h, d], r2.at[h, src], dev(src, z, core))

    def third_copy(h, src, lane):
        return remote(gbufs[h].at[src, lane], gbufs[h].at[src, lane], s3.at[h, src], r3.at[h, src], partner)

    def to_left(h, n):
        return remote(halo.at[h, 0, :, :, LANES[n]], exts[h][n].at[10:12], hs_sem.at[h, 0, n], hr_sem.at[h, 0, n], me - 1)

    def to_right(h, n):
        return remote(halo.at[h, 1, :, :, LANES[n]], exts[h][n].at[8:10], hs_sem.at[h, 1, n], hr_sem.at[h, 1, n], me + 1)

    small = [
        pltpu.make_async_copy(src, dst, in_sem.at[4 + i])
        for i, (src, dst) in enumerate(
            ((deg_hbm, deg), (cols_hbm, cols), (sblk_hbm, sblk), (scnt_hbm, scnt), (hubs_hbm, hubs)))
    ]
    loads = [
        pltpu.make_async_copy(feat, xf, in_sem.at[0]),
        pltpu.make_async_copy(emb, xe, in_sem.at[1]),
        pltpu.make_async_copy(w_hbm, wv, in_sem.at[2]),
        pltpu.make_async_copy(tv_hbm, tv, in_sem.at[3]),
    ]
    barrier = pltpu.get_barrier_semaphore()

    @pl.loop(1, 2 * NZ)
    def _(d):
        pl.semaphore_signal(barrier, inc=1, device_id={"dom": g * 2 * NZ + lax.rem(z * 2 + core + d, 2 * NZ)})

    @pl.loop(1, NG)
    def _(d):
        pl.semaphore_signal(barrier, inc=1, device_id={"dom": dev(plane(d), z, core)})

    @pl.when(me > 0)
    def _():
        pl.semaphore_signal(barrier, inc=1, device_id={"dom": me - 1})

    @pl.when(me < N_DOM - 1)
    def _():
        pl.semaphore_signal(barrier, inc=1, device_id={"dom": me + 1})

    for load in small + loads:
        load.start()

    def barrier_wait():
        extra = jnp.where(me > 0, 1, 0) + jnp.where(me < N_DOM - 1, 1, 0)
        pl.semaphore_wait(barrier, 2 * NZ - 1 + NG - 1 + extra)

    for load in small:
        load.wait()
    root = lax.rsqrt(deg[...].astype(F32))
    for b in range(BLOCKS):
        inv[b] = jnp.broadcast_to(root[b : b + 1, :], (TILE, TILE)).T

    @pl.when(me == 0)
    def _():
        for h in range(HOPS):
            for n, (_, count) in enumerate(CHUNKS):
                exts[h][n][8:10] = jnp.zeros((2, TILE, count), BF16)

    @pl.when(me == N_DOM - 1)
    def _():
        for h in range(HOPS):
            for n, (_, count) in enumerate(CHUNKS):
                exts[h][n][10:12] = jnp.zeros((2, TILE, count), BF16)

    hub_block = [lax.shift_right_logical(hubs[i], 7) for i in range(2)]
    hub_in = [jnp.bitwise_and(hubs[i], TILE - 1) for i in range(2)]

    def pick(ref):
        rows = []
        for i in range(2):
            block = ref[hub_block[i]].astype(F32)
            hit = lax.broadcasted_iota(jnp.int32, block.shape, 0) == hub_in[i]
            rows.append(jnp.sum(jnp.where(hit, block, 0.0), axis=0, keepdims=True))
        return jnp.concatenate(rows, axis=0)

    def times(block, scale):
        width = block.shape[-1]
        return jnp.concatenate([block[:, j : j + TILE] * scale for j in range(0, width, TILE)], axis=1)

    def send_first(h, pair):
        hsend[h] = pair
        if h == 0:
            barrier_wait()

        for d in RING_FAR_FIRST:
            q, copy = first_copy(h, d)

            @pl.when(q != me)
            def _():
                copy.start()

        @pl.when(cls == core)
        def _():
            land[h, own_slot] = pair

    def listed(j, s, width):
        live = lax.broadcasted_iota(jnp.int32, (TILE, width), 0) * 0 + s < scnt[0, j]
        return sblk[0, j, s], live

    def send_halo(h, n):
        @pl.when(me > 0)
        def _():
            to_left(h, n).start()

        @pl.when(me < N_DOM - 1)
        def _():
            to_right(h, n).start()

    hub_scale = pick(inv)
    loads[0].wait()
    loads[1].wait()
    first = jnp.concatenate([pick(xf), pick(xe)], axis=1)
    send_first(0, times(first, hub_scale).astype(BF16))
    for n, (at, count) in enumerate(CHUNKS):
        for j in range(2):
            for s in range(2):
                b, live = listed(j, s, count)
                block = xf[b, :, LANES[n]] if at < F else xe[b]
                halo[0, j, s, :, LANES[n]] = jnp.where(live, times(block.astype(F32), inv[b]), 0.0).astype(BF16)
        send_halo(0, n)

    @pl.loop(0, BLOCKS)
    def _(b):
        scale = inv[b]
        for n, (at, count) in enumerate(CHUNKS):
            block = xf[b, :, LANES[n]] if at < F else xe[b]
            exts[0][n][b] = times(block.astype(F32), scale).astype(BF16)

    loads[2].wait()
    loads[3].wait()
    hub_w = jnp.concatenate([pick(wv), jnp.zeros((14, HUBS), F32)], axis=0).astype(BF16)

    for h in range(HOPS):
        for s in range(NZ):
            source = dev(g, core * HALF_Z + s // 2, s % 2)

            @pl.when(source != me)
            def _():
                remote(hsend.at[h], land.at[h, s], s1.at[h, s], r1.at[h, s], source).wait_recv()

        whole = jnp.concatenate([land[h, s].astype(F32) for s in range(NZ)], axis=0).astype(BF16)
        tsend[h] = whole
        gbufs[h][g, core] = whole

        for d in FAR_FIRST:
            second_copy(h, d).start()
        third_copy(h, g, core).start()

        for n, (at, count) in enumerate(CHUNKS):
            @pl.when(me > 0)
            def _():
                to_right(h, n).wait_recv()

            @pl.when(me < N_DOM - 1)
            def _():
                to_left(h, n).wait_recv()

            @pl.loop(0, BLOCKS, unroll=8)
            def _(b):
                left = jnp.concatenate([tv[b, k] for k in range(K)], axis=1)
                right = jnp.concatenate([exts[h][n][cols[k, b]] for k in range(K)], axis=0)
                acc[b, :, LANES[n]] = jnp.dot(left, right, preferred_element_type=F32)

        for d in FAR_FIRST[::-1]:
            src, landed = arrival(h, d)
            landed.wait_recv()
            third_copy(h, src, core).start()
        if h < HOPS - 1:
            local_hub = pick(acc)

        @pl.loop(0, NG)
        def _(src):
            third_copy(h, src, 1 - core).wait_recv()

        if h == HOPS - 1:
            break

        gathered = gbufs[h][...].reshape(HUBS, WIDTH)
        y = local_hub + jnp.dot(hub_w, gathered, preferred_element_type=F32)[:2]
        x = times(y, hub_scale).astype(BF16)
        send_first(h + 1, times(x.astype(F32), hub_scale).astype(BF16))

        for n, (at, count) in enumerate(CHUNKS):
            picked = [(j, s, *listed(j, s, count)) for j in range(2) for s in range(2)]
            prod = jnp.dot(
                jnp.concatenate([wv[b] for _, _, b, _ in picked], axis=0),
                gbufs[h][:, :, :, LANES[n]].reshape(HUBS, count), preferred_element_type=F32)
            for i, (j, s, b, live) in enumerate(picked):
                scale = inv[b]
                x = times(acc[b, :, LANES[n]] + prod[i * TILE : (i + 1) * TILE], scale).astype(BF16)
                halo[h + 1, j, s, :, LANES[n]] = jnp.where(live, times(x.astype(F32), scale), 0.0).astype(BF16)
            send_halo(h + 1, n)

        for n, (first, count) in enumerate(CHUNKS):
            hub_part = gbufs[h][:, :, :, LANES[n]].reshape(HUBS, count)

            @pl.loop(0, 2, unroll=2)
            def _(half):
                w_rows = wv[pl.ds(half * 4, 4)].reshape(4 * TILE, HUBS)
                prod = jnp.dot(w_rows, hub_part, preferred_element_type=F32)
                for q in range(4):
                    b = half * 4 + q
                    scale = inv[b]
                    for j in range(count // TILE):
                        at = slice(first + j * TILE, first + (j + 1) * TILE)
                        y = acc[b, :, at] + prod[q * TILE : (q + 1) * TILE, j * TILE : (j + 1) * TILE]
                        x = (y * scale).astype(BF16)
                        xo[h, b, :, at] = x
                        exts[h + 1][n][b, :, j * TILE : (j + 1) * TILE] = (x.astype(F32) * scale).astype(BF16)

    for h in range(HOPS):
        @pl.loop(0, NZ)
        def _(d):
            q, copy = first_copy(h, d)

            @pl.when(q != me)
            def _():
                copy.wait_send()

        for d in range(1, NG):
            second_copy(h, d).wait_send()

        @pl.loop(0, NG)
        def _(src):
            third_copy(h, src, core).wait_send()

        for n in range(len(CHUNKS)):
            @pl.when(me > 0)
            def _():
                to_left(h, n).wait_send()

            @pl.when(me < N_DOM - 1)
            def _():
                to_right(h, n).wait_send()


def last(xo, wv, inv, acc, gbuf, outf, oute, x3, sem):
    def put(h, src, first, count, i):
        if first < F:
            dst = outf.at[h, :, :, first : first + count]
        else:
            dst = oute.at[h]
        return pltpu.make_async_copy(src, dst, sem.at[i])

    puts = [put(h, xo.at[h, :, :, first : first + count], first, count, 2 * h + (first > 0))
            for h in range(HOPS - 1) for first, count in ((0, F), (F, E))]
    for p in puts:
        p.start()
    for n, (first, count) in enumerate(CHUNKS):
        lanes = slice(first, first + count)
        hub_part = gbuf[:, :, :, lanes].reshape(HUBS, count)

        @pl.loop(0, 2, unroll=2)
        def _(half):
            w_rows = wv[pl.ds(half * 4, 4)].reshape(4 * TILE, HUBS)
            prod = jnp.dot(w_rows, hub_part, preferred_element_type=F32)
            for q in range(4):
                b = half * 4 + q
                scale = inv[b]
                for j in range(count // TILE):
                    at = slice(first + j * TILE, first + (j + 1) * TILE)
                    y = acc[b, :, at] + prod[q * TILE : (q + 1) * TILE, j * TILE : (j + 1) * TILE]
                    x3[b, :, at] = (y * scale).astype(BF16)

        p = put(HOPS - 1, x3.at[:, :, lanes], first, count, 4 + n)
        p.start()
        puts.append(p)
    for p in puts:
        p.wait()


def body(features, embeddings, tile_values, tile_columns, send_blocks, send_count, hub_rows, hub_weight, degree):
    hbm = pl.BlockSpec(memory_space=pltpu.HBM)
    vmem = pl.BlockSpec(memory_space=pltpu.VMEM)
    dma = pltpu.SemaphoreType.DMA
    outs = [
        ((HOPS - 1, BLOCKS, TILE, WIDTH), BF16),
        ((BLOCKS, TILE, HUBS), BF16),
        ((BLOCKS, TILE, TILE), F32),
        ((BLOCKS, TILE, WIDTH), F32),
        ((NG, 2, 16, WIDTH), BF16),
    ]
    held = pl.pallas_call(
        kernel,
        out_shape=[pltpu.VMEM(*o) for o in outs],
        in_specs=[hbm] * 9,
        out_specs=[vmem] * 5,
        scratch_shapes=[
            pltpu.VMEM((8, 128), jnp.int32),
            pltpu.SMEM((K, BLOCKS), jnp.int32),
            pltpu.SMEM((1, 2, 2), jnp.int32),
            pltpu.SMEM((1, 2), jnp.int32),
            pltpu.SMEM((2,), jnp.int32),
            pltpu.VMEM((BLOCKS, TILE, F), BF16),
            pltpu.VMEM((BLOCKS, TILE, E), BF16),
            pltpu.VMEM((BLOCKS, K, TILE, TILE), BF16),
            *[pltpu.VMEM((12, TILE, count), BF16) for _ in range(HOPS) for _, count in CHUNKS],
            pltpu.VMEM((HOPS, 2, 2, TILE, WIDTH), BF16),
            pltpu.VMEM((HOPS, 2, WIDTH), BF16),
            pltpu.VMEM((HOPS, NZ, 2, WIDTH), BF16),
            pltpu.VMEM((HOPS, 16, WIDTH), BF16),
            pltpu.VMEM((NG, 2, 16, WIDTH), BF16),
            pltpu.VMEM((NG, 2, 16, WIDTH), BF16),
            dma((9,)),
            dma((HOPS, 2, len(CHUNKS))),
            dma((HOPS, 2, len(CHUNKS))),
            dma((HOPS, NZ)),
            dma((HOPS, NZ)),
            dma((HOPS, NG)),
            dma((HOPS, NG)),
            dma((HOPS, NG)),
            dma((HOPS, NG)),
        ],
        compiler_params=pltpu.CompilerParams(
            collective_id=0, has_side_effects=True, vmem_limit_bytes=59_000_000
        ),
        name="hops",
    )(
        features.reshape(BLOCKS, TILE, F), embeddings.reshape(BLOCKS, TILE, E), tile_values,
        hub_weight.reshape(BLOCKS, TILE, HUBS), degree.reshape(8, 128), tile_columns.T,
        send_blocks, send_count, hub_rows,
    )
    outf, oute = pl.pallas_call(
        last,
        out_shape=(
            jax.ShapeDtypeStruct((HOPS, BLOCKS, TILE, F), BF16),
            jax.ShapeDtypeStruct((HOPS, BLOCKS, TILE, E), BF16),
        ),
        in_specs=[vmem] * 5,
        out_specs=(hbm, hbm),
        scratch_shapes=[pltpu.VMEM((BLOCKS, TILE, WIDTH), BF16), dma((7,))],
        compiler_params=pltpu.CompilerParams(vmem_limit_bytes=16 * 1024 * 1024),
        name="last",
    )(*held)
    return outf.reshape(HOPS, ROWS, F), oute.reshape(HOPS, ROWS, E)


def solution(mesh):
    dom = P("dom", None)
    placed = (dom, dom, P("dom", None, None, None), dom, P("dom", None, None), dom, P("dom"), dom, P("dom"))
    return jax.shard_map(
        body,
        mesh=mesh,
        in_specs=placed,
        out_specs=(P(None, "dom", None), P(None, "dom", None)),
        check_vma=False,
    )
```
